32 devices in a mesh: tile: 16 (over z, y, core), head: 2 (over x).
Axes of the slice: x: 2, y: 2, z: 4, core: 2. Of those that a mesh axis runs over, the one named last changes fastest.
Arguments:
- video_q: bfloat16 [8192, 3072], P('tile', 'head'), may hold values from -16 to 16
- video_k: bfloat16 [8192, 3072], P('tile', 'head'), may hold values from -16 to 16
- video_v: bfloat16 [8192, 3072], P('tile', 'head'), may hold values from -12 to 12
- text_q: bfloat16 [256, 3072], P('tile', 'head'), may hold values from -16 to 16
- text_k: bfloat16 [256, 3072], P('tile', 'head'), may hold values from -10 to 10
- text_v: bfloat16 [256, 3072], P('tile', 'head'), may hold values from -12 to 12
- video_proj: bfloat16 [3072, 3072], P('head'), may hold values from -0.109375 to 0.109375
- text_proj: bfloat16 [3072, 3072], P('head'), may hold values from -0.109375 to 0.109375
- window_mask: int32 [32, 27], P('tile'), may hold values from 0 to 1, as said below
- text_length: int32 [1], replicated, may hold values from 64 to 256
Outputs:
- video_out: bfloat16 [8192, 3072], P('tile', 'head')
- text_out: bfloat16 [256, 3072], P('tile', 'head')
The draws below stay inside these ranges and needn't reach their ends.
Inputs may be any that keep to these rules, and one draw needn't show every extreme that they name: window_mask[s, 9 a + 3 b + c] is 1 only if the tile at frame, row and column offsets a - 1, b - 1, c - 1 from tile s lies inside the grid of 2 x 4 x 4 tiles; the centre entry 13 is always 1.
All inputs are finite; a program needn't handle non-finite values.
Results may differ from the reference program's by a relative error of at most 0.013.
Values may be sent and summed in bfloat16 or wider, within the bound.
A program may use at most 320 MiB of HBM per device.

```python
import math
import jax
import jax.numpy as jnp
from jax import lax

D = 3072
HEADS = 24
HD = 128
TILE_TOK = 256
TEXT = 256
GT = 2
BH = 1
BW = 1
DW = 4
GH = 4
GW = 4
TILES_DEV = 2
TILES = 32
VTOK = 8192
N_HEAD = 2


def base_rows(key, draw_tag, row_total):
    sub_key = jax.random.fold_in(key, draw_tag)
    return jnp.clip(1.4 * jax.random.normal(sub_key, (row_total, HEADS * HD), jnp.float32), -8.4, 8.4)


def drawn(key, draw_tag, row_total):
    values = base_rows(key, draw_tag, row_total)
    return values


def draw_video_q(key, part):
    return drawn(key, 11, VTOK).astype(jnp.bfloat16)


def draw_video_k(key, part):
    return drawn(key, 12, VTOK).astype(jnp.bfloat16)


def draw_text_q(key, part):
    return drawn(key, 13, TEXT).astype(jnp.bfloat16)


def draw_window_mask(key, part):
    slot_ids = jnp.arange(TILES, dtype=jnp.int32)
    device_ids = slot_ids // TILES_DEV
    local_ids = slot_ids % TILES_DEV
    frame_ids = local_ids // (BH * BW)
    row_ids = device_ids // DW * BH + local_ids // BW % BH
    col_ids = device_ids % DW * BW + local_ids % BW
    offset = jnp.arange(27, dtype=jnp.int32)
    near_frame = frame_ids[:, None] + offset[None, :] // 9 - 1
    near_row = row_ids[:, None] + offset[None, :] // 3 % 3 - 1
    near_col = col_ids[:, None] + offset[None, :] % 3 - 1
    inside = (near_frame >= 0) & (near_frame < GT) & (near_row >= 0) & (near_row < GH) & (near_col >= 0) & (near_col < GW)
    retained = jax.random.randint(jax.random.fold_in(key, 21), (TILES, 27), 0, 5) > 0
    return (inside & (retained | (offset == 13)[None, :])).astype(jnp.int32)


def block_scale(own_key, extent, pieces, low, top_value):
    factor_of = 1.0
    for axis_at, parts in pieces:
        steps = jax.random.uniform(jax.random.fold_in(jax.random.fold_in(own_key, 6), axis_at), (parts,), jnp.float32, low / len(pieces), top_value / len(pieces))
        factor_of = factor_of * jnp.repeat(jnp.exp(steps), extent[axis_at] // parts).reshape((-1,) + (1,) * (len(extent) - 1 - axis_at))
    return factor_of


def scatter_about(own_key, extent, scale, reach, cuts=(), kind=jnp.bfloat16):
    values = scale * jax.random.normal(own_key, extent, jnp.float32)
    if cuts:
        values = values * block_scale(own_key, extent, cuts, -0.22, 0.18)
    return jnp.clip(values, -reach, reach).astype(kind)


def setup_inputs(seed: int = 0) -> dict:
    keys = jax.random.split(jax.random.key(seed), 11)
    return {
        "video_q": draw_video_q(jax.random.fold_in(keys[10], 71), 0),
        "video_k": draw_video_k(jax.random.fold_in(keys[10], 71), 0),
        "video_v": scatter_about(keys[2], (VTOK, HEADS * HD), 2.0, 12.0, ((0, 16), (1, 2))),
        "text_q": draw_text_q(jax.random.fold_in(keys[10], 71), 0),
        "text_k": scatter_about(keys[4], (TEXT, HEADS * HD), 1.7, 10.0, ((0, 16), (1, 2))),
        "text_v": scatter_about(keys[5], (TEXT, HEADS * HD), 2.0, 12.0, ((0, 16), (1, 2))),
        "video_proj": scatter_about(keys[6], (HEADS * HD, D), (HEADS * HD) ** -0.5, 0.109375, ((0, 2),)),
        "text_proj": scatter_about(keys[7], (HEADS * HD, D), (HEADS * HD) ** -0.5, 0.109375, ((0, 2),)),
        "window_mask": draw_window_mask(jax.random.fold_in(keys[10], 71), 0),
        "text_length": jax.random.randint(keys[9], (1,), TEXT // 4, TEXT + 1).astype(jnp.int32),
    }


NEG_FILL = -1e+30

def attend_tile(queries, window_keys, window_values, key_live, text_keys, text_values, text_live, score_scale):
    near_scores = jnp.einsum('qhd,khd->hqk', queries.astype(jnp.float32), window_keys.astype(jnp.float32)) * score_scale
    near_scores = jnp.where(key_live[None, None, :], near_scores, NEG_FILL)
    text_scores = jnp.einsum('qhd,khd->hqk', queries.astype(jnp.float32), text_keys.astype(jnp.float32)) * score_scale
    text_scores = jnp.where(text_live[None, None, :], text_scores, NEG_FILL)
    row_peak = jnp.maximum(lax.optimization_barrier(jnp.max(near_scores, axis=-1)), lax.optimization_barrier(jnp.max(text_scores, axis=-1)))
    near_weights = jnp.exp(near_scores - row_peak[..., None])
    text_weights = jnp.exp(text_scores - row_peak[..., None])
    weight_sum = lax.optimization_barrier(jnp.sum(near_weights, axis=-1)) + lax.optimization_barrier(jnp.sum(text_weights, axis=-1))
    near_rounded = lax.optimization_barrier(near_weights.astype(jnp.bfloat16)).astype(jnp.float32)
    text_rounded = lax.optimization_barrier(text_weights.astype(jnp.bfloat16)).astype(jnp.float32)
    weighted = jnp.einsum('hqk,khd->hqd', near_rounded, window_values.astype(jnp.float32))
    weighted = weighted + jnp.einsum('hqk,khd->hqd', text_rounded, text_values.astype(jnp.float32))
    result = weighted / weight_sum[..., None]
    return jnp.transpose(result, (1, 0, 2)).reshape(queries.shape[0], -1).astype(jnp.bfloat16)

def project_groups(attended, weight):
    row_total = attended.shape[0]
    group_width = attended.shape[1] // N_HEAD
    grouped = jnp.transpose(attended.reshape(row_total, N_HEAD, group_width), (1, 0, 2))
    weight_groups = weight.reshape(N_HEAD, group_width, weight.shape[1])

    def add_group(running_sum, group_pair):
        partial_sum = jnp.dot(group_pair[0], group_pair[1], preferred_element_type=jnp.float32).astype(jnp.bfloat16)
        partial_sum = lax.optimization_barrier(partial_sum)
        return (running_sum + partial_sum.astype(jnp.float32), None)
    running_sum, unused_out = lax.scan(add_group, jnp.zeros((row_total, weight.shape[1]), jnp.float32), (grouped, weight_groups))
    return running_sum.astype(jnp.bfloat16)

def reference(video_q, video_k, video_v, text_q, text_k, text_v, video_proj, text_proj, window_mask, text_length):
    score_scale = 1.0 / math.sqrt(HD)
    slot_ids = jnp.arange(TILES, dtype=jnp.int32)
    device_ids = slot_ids // TILES_DEV
    local_ids = slot_ids % TILES_DEV
    frame_ids = local_ids // (BH * BW)
    row_ids = device_ids // DW * BH + local_ids // BW % BH
    col_ids = device_ids % DW * BW + local_ids % BW
    offsets = jnp.arange(3, dtype=jnp.int32) - 1
    frame_grid = jnp.broadcast_to(jnp.arange(GT, dtype=jnp.int32)[None, :, None, None], (TILES, GT, 3, 3))
    row_grid = jnp.broadcast_to(jnp.clip(row_ids[:, None, None, None] + offsets[None, None, :, None], 0, GH - 1), (TILES, GT, 3, 3))
    col_grid = jnp.broadcast_to(jnp.clip(col_ids[:, None, None, None] + offsets[None, None, None, :], 0, GW - 1), (TILES, GT, 3, 3))
    neighbour_slots = (row_grid // BH * DW + col_grid // BW) * TILES_DEV + (frame_grid * BH + row_grid % BH) * BW + col_grid % BW
    neighbour_slots = neighbour_slots.reshape(TILES, GT * 9).astype(jnp.int32)
    frame_gap = frame_grid - frame_ids[:, None, None, None] + 1
    mask_column = jnp.clip(frame_gap, 0, 2) * 9 + jnp.broadcast_to((offsets[None, None, :, None] + 1) * 3 + offsets[None, None, None, :] + 1, (TILES, GT, 3, 3))
    mask_column = mask_column.reshape(TILES, GT * 9).astype(jnp.int32)
    tile_live = (jnp.take_along_axis(window_mask, mask_column, axis=1) > 0) & (jnp.abs(frame_gap - 1) <= 1).reshape(TILES, GT * 9)
    tiled_keys = video_k.reshape(TILES, TILE_TOK, HEADS, HD)
    tiled_values = video_v.reshape(TILES, TILE_TOK, HEADS, HD)
    tiled_queries = video_q.reshape(TILES, TILE_TOK, HEADS, HD)
    text_keys = text_k.reshape(TEXT, HEADS, HD)
    text_values = text_v.reshape(TEXT, HEADS, HD)
    text_live = jnp.arange(TEXT, dtype=jnp.int32) < text_length[0]

    def one_tile(slot_index):
        near_keys = tiled_keys[neighbour_slots[slot_index]].reshape(GT * 9 * TILE_TOK, HEADS, HD)
        near_values = tiled_values[neighbour_slots[slot_index]].reshape(GT * 9 * TILE_TOK, HEADS, HD)
        key_live = jnp.repeat(tile_live[slot_index], TILE_TOK)
        return attend_tile(tiled_queries[slot_index], near_keys, near_values, key_live, text_keys, text_values, text_live, score_scale)
    video_attn = lax.map(one_tile, slot_ids).reshape(VTOK, HEADS * HD)

    def head_major(array, count):
        return jnp.transpose(array.reshape(count, HEADS, HD), (1, 0, 2))

    def one_head(head_parts):
        head_query, head_keys, head_values, head_text_keys, head_text_values = head_parts
        near_scores = jnp.dot(head_query, head_keys.T, preferred_element_type=jnp.float32) * score_scale
        text_scores = jnp.dot(head_query, head_text_keys.T, preferred_element_type=jnp.float32) * score_scale
        text_scores = jnp.where(text_live[None, :], text_scores, NEG_FILL)
        row_peak = jnp.maximum(lax.optimization_barrier(jnp.max(near_scores, axis=-1)), lax.optimization_barrier(jnp.max(text_scores, axis=-1)))
        near_weights = jnp.exp(near_scores - row_peak[:, None])
        text_weights = jnp.exp(text_scores - row_peak[:, None])
        weight_sum = lax.optimization_barrier(jnp.sum(near_weights, axis=-1)) + lax.optimization_barrier(jnp.sum(text_weights, axis=-1))
        weighted = jnp.dot(near_weights, head_values.astype(jnp.float32), precision=lax.Precision.HIGHEST)
        weighted = weighted + jnp.dot(text_weights, head_text_values.astype(jnp.float32), precision=lax.Precision.HIGHEST)
        return weighted / weight_sum[:, None]
    text_heads = lax.map(one_head, (head_major(text_q, TEXT), head_major(video_k, VTOK), head_major(video_v, VTOK), head_major(text_k, TEXT), head_major(text_v, TEXT)))
    text_attn = jnp.transpose(text_heads, (1, 0, 2)).reshape(TEXT, HEADS * HD).astype(jnp.bfloat16)
    return (project_groups(video_attn, video_proj), project_groups(text_attn, text_proj))
```

```python
import functools
import math

import jax
import jax.numpy as jnp
from jax import lax
from jax.experimental import pallas as pl
from jax.experimental.pallas import tpu as pltpu
from jax.sharding import PartitionSpec as P

HD = 128
TILE_TOK = 256
GT = 2
DH = 4
NEG_FILL = -1e30
SCALE = 1.0 / math.sqrt(HD)
SCALE2 = SCALE * math.log2(math.e)
CHUNKS = 2


GROUPS = (
    ((0, 0), (-1, 0), (1, 0)),
    ((0, -1), (0, 1)),
    ((-1, -1), (-1, 1), (1, -1), (1, 1)),
)
NEAR = tuple(gap for group in GROUPS for gap in group)

NT = (((1,), (1,)), ((), ()))


def dot_nt(a, b):
    return lax.dot_general(a, b, NT, preferred_element_type=jnp.float32)


def with_ones(values):
    return jnp.concatenate([values, jnp.ones_like(values)], axis=1)


def video_kernel(mask_ref, length_ref, q_ref, *refs):
    near_refs = dict(zip(NEAR, refs[:9]))
    tk_ref, tv_ref, out_ref = refs[9:]
    tiles = q_ref.shape[0] // TILE_TOK
    queries = [q_ref[t * TILE_TOK : (t + 1) * TILE_TOK, :] for t in range(tiles)]
    peak = [None] * tiles
    acc = [None] * tiles
    for number, group in enumerate(GROUPS):
        values = [with_ones(near_refs[gap][1]) for gap in group]
        last = number == len(GROUPS) - 1
        if last:
            text_values = with_ones(tv_ref[...])
        for t in range(tiles):
            parts = []
            maxima = []
            for gap, value in zip(group, values):
                scores = dot_nt(queries[t], near_refs[gap][0])
                for f in range(GT):
                    slot = 9 * (f - t + 1) + 3 * (gap[0] + 1) + gap[1] + 1
                    bias = jnp.where(mask_ref[t, slot] > 0, 0.0, NEG_FILL).astype(jnp.float32)
                    piece = scores[:, f * TILE_TOK : (f + 1) * TILE_TOK]
                    maxima.append(jnp.max(piece, axis=1, keepdims=True) + bias)
                    parts.append((piece, bias, value, f))
            if last:
                scores = dot_nt(queries[t], tk_ref[...])
                live = lax.broadcasted_iota(jnp.int32, scores.shape, 1) < length_ref[0]
                scores = jnp.where(live, scores, NEG_FILL)
                maxima.append(jnp.max(scores, axis=1, keepdims=True))
            new_peak = functools.reduce(jnp.maximum, maxima)
            if peak[t] is not None:
                new_peak = jnp.maximum(peak[t], new_peak)
            shift = new_peak * SCALE2
            total = None
            for at in range(0, len(parts), GT):
                weights = [
                    jnp.exp2(piece * SCALE2 - (shift - bias)).astype(jnp.bfloat16)
                    for piece, bias, _, _ in parts[at : at + GT]
                ]
                term = jnp.dot(
                    jnp.concatenate(weights, axis=1),
                    parts[at][2],
                    preferred_element_type=jnp.float32,
                )
                total = term if total is None else total + term
            if last:
                weights = jnp.exp2(scores * SCALE2 - shift).astype(jnp.bfloat16)
                total = total + jnp.dot(weights, text_values, preferred_element_type=jnp.float32)
            if acc[t] is None:
                acc[t] = total
            else:
                acc[t] = acc[t] * jnp.exp2(peak[t] * SCALE2 - shift) + total
            peak[t] = new_peak
    for t in range(tiles):
        out_ref[t * TILE_TOK : (t + 1) * TILE_TOK, :] = (
            acc[t][:, :HD] / acc[t][:, HD : HD + 1]
        ).astype(jnp.bfloat16)


def video_attention(mask, length, video_q, near, text_k, text_v, first_head, heads):
    rows = video_q.shape[0]
    text = text_k.shape[0]
    smem = pl.BlockSpec(memory_space=pltpu.SMEM)
    own = pl.BlockSpec((rows, HD), lambda h: (0, first_head + h))
    block = pl.BlockSpec((2, rows, HD), lambda h: (0, 0, h))
    token = pl.BlockSpec((text, HD), lambda h: (0, first_head + h))
    keys = 9 * rows + text
    return pl.pallas_call(
        video_kernel,
        grid=(heads,),
        in_specs=[smem, smem, own] + [block] * 9 + [token] * 2,
        out_specs=pl.BlockSpec((rows, HD), lambda h: (0, h)),
        out_shape=jax.ShapeDtypeStruct((rows, heads * HD), jnp.bfloat16),
        compiler_params=pltpu.CompilerParams(vmem_limit_bytes=56 * 1024 * 1024),
        cost_estimate=pl.CostEstimate(
            flops=8 * heads * rows * keys * HD,
            bytes_accessed=heads * keys * HD * 4,
            transcendentals=heads * rows * keys,
        ),
        name="video_attention",
    )(mask, length, video_q, *[near[gap] for gap in NEAR], text_k, text_v)


def text_kernel(first_ref, length_ref, q_ref, k_ref, v_ref, tk_ref, tv_ref, out_ref, lse_ref):
    head = pl.program_id(0)
    queries = q_ref[...]
    scores = dot_nt(queries, k_ref[...])
    own = dot_nt(queries, tk_ref[...])
    live = first_ref[0] + lax.broadcasted_iota(jnp.int32, own.shape, 1) < length_ref[0]
    own = jnp.where(live, own, NEG_FILL)
    peak = jnp.maximum(
        jnp.max(scores, axis=1, keepdims=True), jnp.max(own, axis=1, keepdims=True)
    )
    weights = jnp.exp2((scores - peak) * SCALE2)
    own_weights = jnp.exp2((own - peak) * SCALE2)
    total = jnp.sum(weights, axis=1, keepdims=True) + jnp.sum(own_weights, axis=1, keepdims=True)
    acc = jnp.dot(weights.astype(jnp.bfloat16), v_ref[...], preferred_element_type=jnp.float32)
    acc = acc + jnp.dot(
        own_weights.astype(jnp.bfloat16), tv_ref[...], preferred_element_type=jnp.float32
    )
    out_ref[...] = (acc / total).astype(jnp.bfloat16)
    lse = peak * SCALE + jnp.log(total)

    @pl.when(head == 0)
    def _():
        lse_ref[...] = jnp.zeros_like(lse_ref)

    lane = lax.broadcasted_iota(jnp.int32, lse_ref.shape, 1)
    lse_ref[...] = jnp.where(lane == head, lse, lse_ref[...])


def text_attention(first, length, text_q, video_k, video_v, text_k, text_v):
    rows, width = video_k.shape
    text = text_q.shape[0]
    heads = width // HD
    smem = pl.BlockSpec(memory_space=pltpu.SMEM)

    def column(count):
        return pl.BlockSpec((count, HD), lambda h: (0, h))

    return pl.pallas_call(
        text_kernel,
        grid=(heads,),
        in_specs=[smem, smem, column(text), column(rows), column(rows)]
        + [column(text_k.shape[0])] * 2,
        out_specs=[column(text), pl.BlockSpec((text, HD), lambda h: (0, 0))],
        out_shape=[
            jax.ShapeDtypeStruct((text, width), jnp.bfloat16),
            jax.ShapeDtypeStruct((text, HD), jnp.float32),
        ],
        cost_estimate=pl.CostEstimate(
            flops=8 * heads * rows * text * HD,
            bytes_accessed=4 * rows * width,
            transcendentals=heads * rows * text,
        ),
        name="text_attention",
    )(first, length, text_q, video_k, video_v, text_k, text_v)


def from_gap(block, row_gap, col_gap):
    across = lax.axis_size("tile") // DH
    route = []
    for t in range(lax.axis_size("tile")):
        row, col = t // across + row_gap, t % across + col_gap
        if 0 <= row < DH and 0 <= col < across:
            route.append((row * across + col, t))
    return lax.ppermute(block, "tile", route)


def halo(own):
    near = {(0, 0): own}
    for gap in (-1, 1):
        near[gap, 0] = from_gap(own, gap, 0)
    for gap in (-1, 1):
        near[0, gap] = from_gap(own, 0, gap)
    for row_gap in (-1, 1):
        for gap in (-1, 1):
            near[row_gap, gap] = from_gap(near[row_gap, 0], 0, gap)
    return near


def per_device(
    video_q,
    video_k,
    video_v,
    text_q,
    text_k,
    text_v,
    video_proj,
    text_proj,
    window_mask,
    text_length,
):
    rows, width = video_q.shape
    heads = width // HD
    local = text_q.shape[0]
    devices = lax.axis_size("tile")
    groups = lax.axis_size("head")
    if groups == 2 and devices == 4 * DH and heads % 2 == 0 and rows == GT * TILE_TOK:
        return fused(
            video_q, video_k, video_v, text_q, text_k, text_v, video_proj, text_proj,
            window_mask, text_length,
        )
    chunks = max(c for c in range(1, CHUNKS + 1) if heads % c == 0)
    step = heads // chunks

    text = lax.all_gather(jnp.stack([text_q, text_k, text_v]), "tile", axis=1, tiled=True)
    nears = []
    for c in range(chunks):
        part = slice(c * step * HD, (c + 1) * step * HD)
        nears.append(halo(jnp.stack([video_k[:, part], video_v[:, part]])))

    first = (lax.axis_index("tile") * local).astype(jnp.int32).reshape(1)
    text_part, text_lse = text_attention(
        first, text_length, text[0], video_k, video_v, text_k, text_v
    )
    text_part = lax.all_to_all(
        text_part.reshape(devices, local, width), "tile", split_axis=0, concat_axis=0
    )
    text_lse = lax.all_to_all(
        text_lse.reshape(devices, local, HD), "tile", split_axis=0, concat_axis=0
    )[:, :, :heads]
    share = jax.nn.softmax(text_lse, axis=0)
    text_attn = jnp.sum(
        share[..., None] * text_part.reshape(devices, local, heads, HD).astype(jnp.float32), axis=0
    )
    text_attn = text_attn.reshape(local, width).astype(jnp.bfloat16)

    results = [
        video_attention(
            window_mask, text_length, video_q, near, text[1], text[2], c * step, step
        )
        for c, near in enumerate(nears)
    ]
    video_attn = jnp.concatenate(results, axis=1)
    return (
        project(video_attn, video_proj, groups),
        project(text_attn, text_proj, groups),
    )


def project(attn, proj, groups):
    if groups != 2:
        part = jnp.dot(attn, proj, preferred_element_type=jnp.float32).astype(jnp.bfloat16)
        return lax.psum_scatter(part, "head", scatter_dimension=1, tiled=True)
    half = proj.shape[1] // groups
    me = lax.axis_index("head")
    theirs = lax.dynamic_slice_in_dim(proj, (1 - me) * half, half, 1)
    mine = lax.dynamic_slice_in_dim(proj, me * half, half, 1)
    away = jnp.dot(attn, theirs, preferred_element_type=jnp.float32).astype(jnp.bfloat16)
    arrived = lax.ppermute(away, "head", [(0, 1), (1, 0)])
    home = jnp.dot(attn, mine, preferred_element_type=jnp.float32).astype(jnp.bfloat16)
    return (home.astype(jnp.float32) + arrived.astype(jnp.float32)).astype(jnp.bfloat16)


def fused_kernel(
    bias_ref, length_ref, q_ref, k_ref, v_ref, tq_ref, tk_ref, tv_ref, vproj_ref, tproj_ref,
    vout_ref, tout_ref,
    qb, kb, vb, tb, biasb, peakb, accb, obuf, hp, xa, wh, wa, tw, tpart, tlse, trecv, tlrecv, ta,
    tsend, tarrive,
    local_sem, pair_send, pair_recv, z_send, z_recv, y_send, y_recv, fy_send, fz_send, d_recv,
    th_send, th_recv, ty_send, ty_recv, ta_send, ta_recv, tl_send, tl_recv,
    w_send, w_recv, wf_send, wf_recv, op_send, op_recv, ox_send, ox_recv, tx_send, tx_recv,
):
    rows, width = q_ref.shape
    half = width // 2
    heads = half // HD
    local = tq_ref.shape[0]
    text = tb.shape[1]
    out_width = vout_ref.shape[1]
    across = lax.axis_size("tile") // DH
    tiles = rows // TILE_TOK
    chips = lax.axis_size("tile") // 2

    me = lax.axis_index("tile")
    group = lax.axis_index("head")
    r = me // across
    yc = me % across // 2
    c = me % 2
    inner = 1 - yc
    chip = r * 2 + yc
    has_lo = r > 0
    has_hi = r < DH - 1

    def at(row, ycol, core):
        return (row * across + 2 * ycol + core, group)

    partner = at(r, yc, 1 - c)
    sides = (k_ref, v_ref)
    bufs = (kb, vb)

    def lanes(h):
        return pl.ds(pl.multiple_of(h * HD, HD), HD)

    def half_lanes(core):
        return pl.ds(pl.multiple_of(core * half, HD), half)

    def remote(src, dst, send, recv, device):
        return pltpu.make_async_remote_copy(
            src_ref=src, dst_ref=dst, send_sem=send, recv_sem=recv, device_id=device,
            device_id_type=pl.DeviceIdType.MESH,
        )

    def arrived(dst, recv):
        remote(dst, dst, pair_send.at[0], recv, partner).wait_recv()

    def z_copy(kv, d, core, h):
        slot = (2 if d else 4) + c
        return remote(
            sides[kv].at[:, lanes(core * heads + h)], bufs[kv].at[slot, :, lanes(h)],
            z_send.at[kv, d, core, h], z_recv.at[kv, slot - 2, h],
            at(r + (1 if d else -1), yc, core),
        )

    def y_copy(kv, core, h):
        return remote(
            sides[kv].at[:, lanes(core * heads + h)], bufs[kv].at[6, :, lanes(h)],
            y_send.at[kv, core, h], y_recv.at[kv, h], at(r, 1 - yc, core),
        )

    def fy_copy(kv, d, h):
        return remote(
            bufs[kv].at[(4 if d else 2) + inner, :, lanes(h)], bufs[kv].at[7 + d, :, lanes(h)],
            fy_send.at[kv, d, h], d_recv.at[kv, d, h], at(r, 1 - yc, c),
        )

    def fz_copy(kv, d, h):
        return remote(
            bufs[kv].at[6, :, lanes(h)], bufs[kv].at[7 + d, :, lanes(h)],
            fz_send.at[kv, d, h], d_recv.at[kv, d, h], at(r + (-1 if d else 1), yc, c),
        )

    def each_z(h, act):
        for d, ok in ((1, has_hi), (0, has_lo)):
            @pl.when(ok)
            def _():
                for kv in range(2):
                    for core in range(2):
                        act(z_copy(kv, d, core, h))

    def each_y(h, act):
        @pl.when(c == inner)
        def _():
            for kv in range(2):
                for core in range(2):
                    act(y_copy(kv, core, h))

    def each_fy(h, act):
        for d, ok in ((0, has_lo), (1, has_hi)):
            @pl.when(ok & (h % 3 != 1 + d))
            def _():
                for kv in range(2):
                    act(fy_copy(kv, d, h))

    def each_fz(h, act):
        for d, ok in ((0, has_hi), (1, has_lo)):
            @pl.when(ok & (h % 3 == 1 + d))
            def _():
                for kv in range(2):
                    act(fz_copy(kv, d, h))

    def start(copy):
        copy.start()

    def sent(copy):
        copy.wait_send()

    def piece(row, ycol):
        return tb.at[:, pl.ds(pl.multiple_of((row * 2 + ycol) * 2 * local, 2 * local), 2 * local), :]

    def th_copy(row, d):
        return remote(
            piece(row, yc), piece(row, yc), th_send.at[row, d], th_recv.at[row],
            at(r + (1 if d else -1), yc, c),
        )

    def ty_copy(row):
        return remote(
            piece(row, yc), piece(row, yc), ty_send.at[row], ty_recv.at[row], at(r, 1 - yc, c)
        )

    mine = pl.ds(pl.multiple_of(me * local, local), local)
    texts = (tq_ref, tk_ref, tv_ref)
    local_copies = [
        pltpu.make_async_copy(texts[i].at[:, half_lanes(c)], tb.at[i, mine, :], local_sem.at[i])
        for i in range(3)
    ]
    pair_copies = [
        remote(
            texts[i].at[:, half_lanes(1 - c)], tb.at[i, mine, :], pair_send.at[i],
            pair_recv.at[i], partner,
        )
        for i in range(3)
    ]
    for dst, src, i in ((kb.at[c], k_ref, 3), (vb.at[c], v_ref, 4), (qb.at[c], q_ref, 5)):
        local_copies.append(
            pltpu.make_async_copy(src.at[:, half_lanes(c)], dst, local_sem.at[i])
        )
        pair_copies.append(
            remote(src.at[:, half_lanes(1 - c)], dst, pair_send.at[i], pair_recv.at[i], partner)
        )
    pair_copies.append(
        remote(bias_ref, biasb.at[c], pair_send.at[6], pair_recv.at[6], partner)
    )
    theirs = pl.ds(pl.multiple_of((me + 1 - 2 * c) * local, local), local)
    pair_targets = [tb.at[i, theirs, :] for i in range(3)] + [
        kb.at[1 - c], vb.at[1 - c], qb.at[1 - c], biasb.at[1 - c]
    ]
    home_copy = pltpu.make_async_copy(
        vproj_ref.at[:, pl.ds(pl.multiple_of(group * out_width, HD), out_width)], wh,
        local_sem.at[6],
    )
    tw_copy = pltpu.make_async_copy(tproj_ref, tw, local_sem.at[7])
    w_rows = pl.ds(pl.multiple_of(c * half, HD), half)
    w_copy = remote(
        vproj_ref.at[w_rows, pl.ds(pl.multiple_of((1 - group) * out_width, HD), out_width)],
        wa.at[w_rows, :], w_send.at[0], w_recv.at[0], (me, 1 - group),
    )
    wf_copy = remote(wa.at[w_rows, :], wa.at[w_rows, :], wf_send.at[0], wf_recv.at[0], partner)

    for i in range(3):
        local_copies[i].start()
        pair_copies[i].start()
    w_copy.start()
    for i in range(3, 6):
        local_copies[i].start()
        pair_copies[i].start()
    pair_copies[6].start()
    biasb[c] = bias_ref[...]

    def hop(row, up, down):
        for ok, d in ((up, 1), (down, 0)):
            @pl.when(ok)
            def _():
                th_copy(row, d).start()
        ty_copy(row).start()

    for i in range(3):
        local_copies[i].wait()
        arrived(pair_targets[i], pair_recv.at[i])
    hop(r, has_hi, has_lo)
    each_z(0, start)
    each_y(0, start)
    for k in range(1, DH):
        @pl.when(r >= k)
        def _():
            arrived(piece(r - k, yc), th_recv.at[r - k])
            hop(r - k, has_hi, False)

        @pl.when(r + k < DH)
        def _():
            arrived(piece(r + k, yc), th_recv.at[r + k])
            hop(r + k, False, has_lo)

        if k == 1:
            each_z(1, start)
            each_y(1, start)
    for i in range(3, 6):
        local_copies[i].wait()
    for i in range(3, 7):
        arrived(pair_targets[i], pair_recv.at[i])
    home_copy.start()
    tw_copy.start()
    for row in range(DH):
        arrived(piece(row, 1 - yc), ty_recv.at[row])

    length = length_ref[0]
    first = chip * 2 * local
    tlse[...] = jnp.zeros_like(tlse)

    @pl.loop(0, heads)
    def _(h):
        queries = tb[0, :, lanes(h)]
        own_keys = [kb[0, :, lanes(h)], kb[1, :, lanes(h)]]
        scores = [dot_nt(queries, keys) for keys in own_keys]
        own = dot_nt(queries, tb[1, :, lanes(h)])
        index = lax.broadcasted_iota(jnp.int32, own.shape, 1)
        live = (index >= first) & (index < first + 2 * local) & (index < length)
        own = jnp.where(live, own, NEG_FILL)
        peak = jnp.max(own, axis=1, keepdims=True)
        for s in scores:
            peak = jnp.maximum(peak, jnp.max(s, axis=1, keepdims=True))
        weights = [jnp.exp2((s - peak) * SCALE2) for s in scores + [own]]
        total = sum(jnp.sum(w, axis=1, keepdims=True) for w in weights)
        values = [vb[0, :, lanes(h)], vb[1, :, lanes(h)], tb[2, :, lanes(h)]]
        acc = sum(
            jnp.dot(w.astype(jnp.bfloat16), v, preferred_element_type=jnp.float32)
            for w, v in zip(weights, values)
        )
        tpart[:, lanes(h)] = (acc / total).astype(jnp.bfloat16)
        lse = peak * SCALE + jnp.log(total)
        lane = lax.broadcasted_iota(jnp.int32, tlse.shape, 1)
        tlse[...] = jnp.where(lane == h, lse, tlse[...])

    def part_rows(d):
        return pl.ds(pl.multiple_of(d * local, local), local)

    def part_copy(d):
        return remote(
            tpart.at[part_rows(d), :], trecv.at[chip, c], ta_send.at[d], ta_recv.at[chip, c],
            (d, group),
        )

    def lse_copy(d):
        return remote(
            tlse.at[part_rows(d), :], tlrecv.at[chip, c], tl_send.at[d], tl_recv.at[chip, c],
            (d, group),
        )

    @pl.loop(0, 2 * chips)
    def _(d):
        @pl.when(d != me)
        def _():
            part_copy(d).start()
            lse_copy(d).start()

    trecv[chip, c] = tpart[mine, :]
    tlrecv[chip, c] = tlse[mine, :]

    def attend(h, q, blocks, with_text, first_group):
        hs = lanes(h)
        values = [with_ones(vb[slot, :, hs]) for slot, _, _ in blocks]
        if with_text:
            text_values = with_ones(tb[2, :, hs])
        for t in range(tiles):
            queries = qb[q, t * TILE_TOK : (t + 1) * TILE_TOK, hs]
            parts = []
            maxima = []
            for (slot, row_gap, col_gap), value in zip(blocks, values):
                scores = dot_nt(queries, kb[slot, :, hs])
                for f in range(GT):
                    column = 27 * t + 9 * (f - t + 1) + 3 * (row_gap + 1) + col_gap + 1
                    bias = biasb[q, pl.ds(column, 1), 0:1]
                    piece_ = scores[:, f * TILE_TOK : (f + 1) * TILE_TOK]
                    maxima.append(jnp.max(piece_, axis=1, keepdims=True) + bias)
                    parts.append((piece_, bias, value))
            if with_text:
                scores = dot_nt(queries, tb[1, :, hs])
                live = lax.broadcasted_iota(jnp.int32, scores.shape, 1) < length
                scores = jnp.where(live, scores, NEG_FILL)
                maxima.append(jnp.max(scores, axis=1, keepdims=True))
            peak = functools.reduce(jnp.maximum, maxima)
            if not first_group:
                old = peakb[q, t, :, 0:1]
                peak = jnp.maximum(old, peak)
            shift = peak * SCALE2
            total = None
            for at_ in range(0, len(parts), GT):
                weights = [
                    jnp.exp2(p * SCALE2 - (shift - b)).astype(jnp.bfloat16)
                    for p, b, _ in parts[at_ : at_ + GT]
                ]
                term = jnp.dot(
                    jnp.concatenate(weights, axis=1), parts[at_][2],
                    preferred_element_type=jnp.float32,
                )
                total = term if total is None else total + term
            if with_text:
                weights = jnp.exp2(scores * SCALE2 - shift).astype(jnp.bfloat16)
                total = total + jnp.dot(
                    weights, text_values, preferred_element_type=jnp.float32
                )
            if not first_group:
                total = accb[q, t] * jnp.exp2(old * SCALE2 - shift) + total
            accb[q, t] = total
            peakb[q, t] = jnp.broadcast_to(peak, peakb.shape[2:])

    def op_copy(h):
        return remote(
            obuf.at[1 - c, :, lanes(h)], hp.at[:, lanes(h)], op_send.at[h], op_recv.at[h], partner
        )

    def ox_copy(core, h):
        return remote(
            obuf.at[core, :, lanes(h)], xa.at[c, :, lanes(h)], ox_send.at[core, h],
            ox_recv.at[c, h], (at(r, yc, core)[0], 1 - group),
        )

    tx_copy = remote(
        tsend, tarrive, tx_send.at[0], tx_recv.at[0], (me, 1 - group)
    )

    def finish_text():
        @pl.loop(0, 2 * chips)
        def _(d):
            @pl.when(d != me)
            def _():
                arrived(trecv.at[d // 2, d % 2], ta_recv.at[d // 2, d % 2])
                arrived(tlrecv.at[d // 2, d % 2], tl_recv.at[d // 2, d % 2])

        for core in range(2):
            lse = [tlrecv[s, core] for s in range(chips)]
            top = functools.reduce(jnp.maximum, lse)
            share = [jnp.exp(l - top) for l in lse]
            whole = sum(share)
            share = [s / whole for s in share]
            for j in range(heads):
                cols = slice(j * HD, (j + 1) * HD)
                acc = sum(
                    share[s][:, j : j + 1] * trecv[s, core, :, cols].astype(jnp.float32)
                    for s in range(chips)
                )
                ta[:, core * half + j * HD : core * half + (j + 1) * HD] = acc.astype(jnp.bfloat16)
        tw_copy.wait()

        @pl.loop(0, out_width // half)
        def _(n):
            cols = pl.ds(pl.multiple_of(n * half, HD), half)
            away = pl.ds(pl.multiple_of((1 - group) * out_width + n * half, HD), half)
            tsend[:, cols] = jnp.dot(
                ta[...], tw[:, away], preferred_element_type=jnp.float32
            ).astype(jnp.bfloat16)

        tx_copy.start()

    arrived(kb.at[6, :, lanes(0)], y_recv.at[0, 0])
    arrived(vb.at[6, :, lanes(0)], y_recv.at[1, 0])

    @pl.loop(0, heads)
    def _(h):
        @pl.when(h + 1 < heads)
        def _():
            for kv in range(2):
                arrived(bufs[kv].at[6, :, lanes(h + 1)], y_recv.at[kv, h + 1])
            each_fz(h + 1, start)

        @pl.when(h + 2 < heads)
        def _():
            each_z(h + 2, start)
            each_y(h + 2, start)

        for ok, slots in ((has_lo, (2, 3)), (has_hi, (4, 5))):
            @pl.when(ok)
            def _():
                for kv in range(2):
                    for slot in slots:
                        arrived(bufs[kv].at[slot, :, lanes(h)], z_recv.at[kv, slot - 2, h])

        each_fy(h, start)

        @pl.when(h == heads - 2)
        def _():
            arrived(wa.at[w_rows, :], w_recv.at[0])
            wf_copy.start()
            finish_text()

        @pl.loop(0, 2)
        def _(q):
            attend(h, q, [(0, 0, -q), (1, 0, 1 - q)], True, True)

            @pl.when(has_lo)
            def _():
                attend(h, q, [(2, -1, -q), (3, -1, 1 - q)], False, False)

            @pl.when(has_hi)
            def _():
                attend(h, q, [(4, 1, -q), (5, 1, 1 - q)], False, False)

        side = 1 - 2 * yc
        attend(h, inner, [(6, 0, side)], False, False)
        for d, ok in ((0, has_lo), (1, has_hi)):
            @pl.when(ok)
            def _():
                for kv in range(2):
                    arrived(bufs[kv].at[7 + d, :, lanes(h)], d_recv.at[kv, d, h])
                attend(h, inner, [(7 + d, 2 * d - 1, side)], False, False)

        @pl.loop(0, 2)
        def _(q):
            for t in range(tiles):
                acc = accb[q, t]
                obuf[q, t * TILE_TOK : (t + 1) * TILE_TOK, lanes(h)] = (
                    acc[:, :HD] / acc[:, HD : HD + 1]
                ).astype(jnp.bfloat16)

        ox_copy(0, h).start()
        ox_copy(1, h).start()
        op_copy(h).start()

    home_copy.wait()
    other = pl.ds(pl.multiple_of((1 - c) * half, HD), half)
    arrived(wa.at[other, :], wf_recv.at[0])

    @pl.loop(0, heads)
    def _(h):
        arrived(hp.at[:, lanes(h)], op_recv.at[h])
        for core in range(2):
            arrived(xa.at[core, :, lanes(h)], ox_recv.at[core, h])

    @pl.loop(0, out_width // TILE_TOK)
    def _(n):
        cols = pl.ds(pl.multiple_of(n * TILE_TOK, HD), TILE_TOK)
        home = jnp.dot(obuf[c], wh[w_rows, cols], preferred_element_type=jnp.float32)
        home = home + jnp.dot(hp[...], wh[other, cols], preferred_element_type=jnp.float32)
        away = jnp.dot(xa[0], wa[:half, cols], preferred_element_type=jnp.float32)
        away = away + jnp.dot(xa[1], wa[half:, cols], preferred_element_type=jnp.float32)
        vout_ref[:, cols] = (
            home.astype(jnp.bfloat16).astype(jnp.float32)
            + away.astype(jnp.bfloat16).astype(jnp.float32)
        ).astype(jnp.bfloat16)

    arrived(tarrive, tx_recv.at[0])

    @pl.loop(0, out_width // half)
    def _(n):
        cols = pl.ds(pl.multiple_of(n * half, HD), half)
        here = pl.ds(pl.multiple_of(group * out_width + n * half, HD), half)
        home = jnp.dot(ta[...], tw[:, here], preferred_element_type=jnp.float32)
        tout_ref[:, cols] = (
            home.astype(jnp.bfloat16).astype(jnp.float32) + tarrive[:, cols].astype(jnp.float32)
        ).astype(jnp.bfloat16)

    for copy in pair_copies:
        copy.wait_send()
    w_copy.wait_send()
    wf_copy.wait_send()
    tx_copy.wait_send()
    for row in range(DH):
        ty_copy(row).wait_send()

        @pl.when(has_hi & (row <= r))
        def _():
            th_copy(row, 1).wait_send()

        @pl.when(has_lo & (row >= r))
        def _():
            th_copy(row, 0).wait_send()

    @pl.loop(0, 2 * chips)
    def _(d):
        @pl.when(d != me)
        def _():
            part_copy(d).wait_send()
            lse_copy(d).wait_send()

    @pl.loop(0, heads)
    def _(h):
        each_z(h, sent)
        each_y(h, sent)
        each_fy(h, sent)
        each_fz(h, sent)
        ox_copy(0, h).wait_send()
        ox_copy(1, h).wait_send()
        op_copy(h).wait_send()


def fused(
    video_q, video_k, video_v, text_q, text_k, text_v, video_proj, text_proj, window_mask,
    text_length,
):
    rows, width = video_q.shape
    half = width // 2
    heads = half // HD
    local = text_q.shape[0]
    devices = lax.axis_size("tile")
    chips = devices // 2
    text = devices * local
    out_width = video_proj.shape[1] // lax.axis_size("head")
    tiles = rows // TILE_TOK
    slots = window_mask.size
    bias = jnp.where(window_mask > 0, 0.0, NEG_FILL).astype(jnp.float32)
    bias = jnp.broadcast_to(bias.reshape(slots, 1), (slots, HD))
    bias = jnp.pad(bias, ((0, -slots % 8), (0, 0)))
    bf16 = jnp.bfloat16
    f32 = jnp.float32
    anywhere = pl.BlockSpec(memory_space=pl.ANY)
    vmem = pl.BlockSpec(memory_space=pltpu.VMEM)
    dma = pltpu.SemaphoreType.DMA
    return pl.pallas_call(
        fused_kernel,
        in_specs=[vmem, pl.BlockSpec(memory_space=pltpu.SMEM)] + [anywhere] * 8,
        out_specs=[vmem, vmem],
        out_shape=[
            jax.ShapeDtypeStruct((rows, out_width), bf16),
            jax.ShapeDtypeStruct((local, out_width), bf16),
        ],
        scratch_shapes=[
            pltpu.VMEM((2, rows, half), bf16),
            pltpu.VMEM((9, rows, half), bf16),
            pltpu.VMEM((9, rows, half), bf16),
            pltpu.VMEM((3, text, half), bf16),
            pltpu.VMEM((2,) + bias.shape, f32),
            pltpu.VMEM((2, tiles, TILE_TOK, HD), f32),
            pltpu.VMEM((2, tiles, TILE_TOK, 2 * HD), f32),
            pltpu.VMEM((2, rows, half), bf16),
            pltpu.VMEM((rows, half), bf16),
            pltpu.VMEM((2, rows, half), bf16),
            pltpu.VMEM((width, out_width), bf16),
            pltpu.VMEM((width, out_width), bf16),
            pltpu.VMEM(text_proj.shape, bf16),
            pltpu.VMEM((text, half), bf16),
            pltpu.VMEM((text, HD), f32),
            pltpu.VMEM((chips, 2, local, half), bf16),
            pltpu.VMEM((chips, 2, local, HD), f32),
            pltpu.VMEM((local, width), bf16),
            pltpu.VMEM((local, out_width), bf16),
            pltpu.VMEM((local, out_width), bf16),
            dma((8,)), dma((7,)), dma((7,)),
            dma((2, 2, 2, heads)), dma((2, 4, heads)),
            dma((2, 2, heads)), dma((2, heads)),
            dma((2, 2, heads)), dma((2, 2, heads)), dma((2, 2, heads)),
            dma((DH, 2)), dma((DH,)), dma((DH,)), dma((DH,)),
            dma((devices,)), dma((chips, 2)), dma((devices,)), dma((chips, 2)),
            dma((1,)), dma((1,)), dma((1,)), dma((1,)),
            dma((heads,)), dma((heads,)), dma((2, heads)), dma((2, heads)),
            dma((1,)), dma((1,)),
        ],
        compiler_params=pltpu.CompilerParams(
            vmem_limit_bytes=60 * 1024 * 1024, has_side_effects=True
        ),
        name="fused",
    )(
        bias, text_length, video_q, video_k, video_v, text_q, text_k, text_v, video_proj,
        text_proj,
    )


def solution(mesh):
    placed = (P("tile", "head"),) * 6 + (P("head", None),) * 2 + (P("tile", None), P())
    return jax.shard_map(
        per_device,
        mesh=mesh,
        in_specs=placed,
        out_specs=(P("tile", "head"), P("tile", "head")),
        check_vma=False,
    )
```

```python
import functools
import math

import jax
import jax.numpy as jnp
from jax import lax
from jax.experimental import pallas as pl
from jax.experimental.pallas import tpu as pltpu
from jax.sharding import PartitionSpec as P

HD = 128
TILE_TOK = 256
GT = 2
DH = 4
NEG_FILL = -1e30
SCALE = 1.0 / math.sqrt(HD)
SCALE2 = SCALE * math.log2(math.e)
CHUNKS = 2


GROUPS = (
    ((0, 0), (-1, 0), (1, 0)),
    ((0, -1), (0, 1)),
    ((-1, -1), (-1, 1), (1, -1), (1, 1)),
)
NEAR = tuple(gap for group in GROUPS for gap in group)

NT = (((1,), (1,)), ((), ()))


def dot_nt(a, b):
    return lax.dot_general(a, b, NT, preferred_element_type=jnp.float32)


def with_ones(values):
    return jnp.concatenate([values, jnp.ones_like(values)], axis=1)


def video_kernel(mask_ref, length_ref, q_ref, *refs):
    near_refs = dict(zip(NEAR, refs[:9]))
    tk_ref, tv_ref, out_ref = refs[9:]
    tiles = q_ref.shape[0] // TILE_TOK
    queries = [q_ref[t * TILE_TOK : (t + 1) * TILE_TOK, :] for t in range(tiles)]
    peak = [None] * tiles
    acc = [None] * tiles
    for number, group in enumerate(GROUPS):
        values = [with_ones(near_refs[gap][1]) for gap in group]
        last = number == len(GROUPS) - 1
        if last:
            text_values = with_ones(tv_ref[...])
        for t in range(tiles):
            parts = []
            maxima = []
            for gap, value in zip(group, values):
                scores = dot_nt(queries[t], near_refs[gap][0])
                for f in range(GT):
                    slot = 9 * (f - t + 1) + 3 * (gap[0] + 1) + gap[1] + 1
                    bias = jnp.where(mask_ref[t, slot] > 0, 0.0, NEG_FILL).astype(jnp.float32)
                    piece = scores[:, f * TILE_TOK : (f + 1) * TILE_TOK]
                    maxima.append(jnp.max(piece, axis=1, keepdims=True) + bias)
                    parts.append((piece, bias, value, f))
            if last:
                scores = dot_nt(queries[t], tk_ref[...])
                live = lax.broadcasted_iota(jnp.int32, scores.shape, 1) < length_ref[0]
                scores = jnp.where(live, scores, NEG_FILL)
                maxima.append(jnp.max(scores, axis=1, keepdims=True))
            new_peak = functools.reduce(jnp.maximum, maxima)
            if peak[t] is not None:
                new_peak = jnp.maximum(peak[t], new_peak)
            shift = new_peak * SCALE2
            total = None
            for at in range(0, len(parts), GT):
                weights = [
                    jnp.exp2(piece * SCALE2 - (shift - bias)).astype(jnp.bfloat16)
                    for piece, bias, _, _ in parts[at : at + GT]
                ]
                term = jnp.dot(
                    jnp.concatenate(weights, axis=1),
                    parts[at][2],
                    preferred_element_type=jnp.float32,
                )
                total = term if total is None else total + term
            if last:
                weights = jnp.exp2(scores * SCALE2 - shift).astype(jnp.bfloat16)
                total = total + jnp.dot(weights, text_values, preferred_element_type=jnp.float32)
            if acc[t] is None:
                acc[t] = total
            else:
                acc[t] = acc[t] * jnp.exp2(peak[t] * SCALE2 - shift) + total
            peak[t] = new_peak
    for t in range(tiles):
        out_ref[t * TILE_TOK : (t + 1) * TILE_TOK, :] = (
            acc[t][:, :HD] / acc[t][:, HD : HD + 1]
        ).astype(jnp.bfloat16)


def video_attention(mask, length, video_q, near, text_k, text_v, first_head, heads):
    rows = video_q.shape[0]
    text = text_k.shape[0]
    smem = pl.BlockSpec(memory_space=pltpu.SMEM)
    own = pl.BlockSpec((rows, HD), lambda h: (0, first_head + h))
    block = pl.BlockSpec((2, rows, HD), lambda h: (0, 0, h))
    token = pl.BlockSpec((text, HD), lambda h: (0, first_head + h))
    keys = 9 * rows + text
    return pl.pallas_call(
        video_kernel,
        grid=(heads,),
        in_specs=[smem, smem, own] + [block] * 9 + [token] * 2,
        out_specs=pl.BlockSpec((rows, HD), lambda h: (0, h)),
        out_shape=jax.ShapeDtypeStruct((rows, heads * HD), jnp.bfloat16),
        compiler_params=pltpu.CompilerParams(vmem_limit_bytes=56 * 1024 * 1024),
        cost_estimate=pl.CostEstimate(
            flops=8 * heads * rows * keys * HD,
            bytes_accessed=heads * keys * HD * 4,
            transcendentals=heads * rows * keys,
        ),
        name="video_attention",
    )(mask, length, video_q, *[near[gap] for gap in NEAR], text_k, text_v)


def text_kernel(first_ref, length_ref, q_ref, k_ref, v_ref, tk_ref, tv_ref, out_ref, lse_ref):
    head = pl.program_id(0)
    queries = q_ref[...]
    scores = dot_nt(queries, k_ref[...])
    own = dot_nt(queries, tk_ref[...])
    live = first_ref[0] + lax.broadcasted_iota(jnp.int32, own.shape, 1) < length_ref[0]
    own = jnp.where(live, own, NEG_FILL)
    peak = jnp.maximum(
        jnp.max(scores, axis=1, keepdims=True), jnp.max(own, axis=1, keepdims=True)
    )
    weights = jnp.exp2((scores - peak) * SCALE2)
    own_weights = jnp.exp2((own - peak) * SCALE2)
    total = jnp.sum(weights, axis=1, keepdims=True) + jnp.sum(own_weights, axis=1, keepdims=True)
    acc = jnp.dot(weights.astype(jnp.bfloat16), v_ref[...], preferred_element_type=jnp.float32)
    acc = acc + jnp.dot(
        own_weights.astype(jnp.bfloat16), tv_ref[...], preferred_element_type=jnp.float32
    )
    out_ref[...] = (acc / total).astype(jnp.bfloat16)
    lse = peak * SCALE + jnp.log(total)

    @pl.when(head == 0)
    def _():
        lse_ref[...] = jnp.zeros_like(lse_ref)

    lane = lax.broadcasted_iota(jnp.int32, lse_ref.shape, 1)
    lse_ref[...] = jnp.where(lane == head, lse, lse_ref[...])


def text_attention(first, length, text_q, video_k, video_v, text_k, text_v):
    rows, width = video_k.shape
    text = text_q.shape[0]
    heads = width // HD
    smem = pl.BlockSpec(memory_space=pltpu.SMEM)

    def column(count):
        return pl.BlockSpec((count, HD), lambda h: (0, h))

    return pl.pallas_call(
        text_kernel,
        grid=(heads,),
        in_specs=[smem, smem, column(text), column(rows), column(rows)]
        + [column(text_k.shape[0])] * 2,
        out_specs=[column(text), pl.BlockSpec((text, HD), lambda h: (0, 0))],
        out_shape=[
            jax.ShapeDtypeStruct((text, width), jnp.bfloat16),
            jax.ShapeDtypeStruct((text, HD), jnp.float32),
        ],
        cost_estimate=pl.CostEstimate(
            flops=8 * heads * rows * text * HD,
            bytes_accessed=4 * rows * width,
            transcendentals=heads * rows * text,
        ),
        name="text_attention",
    )(first, length, text_q, video_k, video_v, text_k, text_v)


def from_gap(block, row_gap, col_gap):
    across = lax.axis_size("tile") // DH
    route = []
    for t in range(lax.axis_size("tile")):
        row, col = t // across + row_gap, t % across + col_gap
        if 0 <= row < DH and 0 <= col < across:
            route.append((row * across + col, t))
    return lax.ppermute(block, "tile", route)


def halo(own):
    near = {(0, 0): own}
    for gap in (-1, 1):
        near[gap, 0] = from_gap(own, gap, 0)
    for gap in (-1, 1):
        near[0, gap] = from_gap(own, 0, gap)
    for row_gap in (-1, 1):
        for gap in (-1, 1):
            near[row_gap, gap] = from_gap(near[row_gap, 0], 0, gap)
    return near


def per_device(
    video_q,
    video_k,
    video_v,
    text_q,
    text_k,
    text_v,
    video_proj,
    text_proj,
    window_mask,
    text_length,
):
    rows, width = video_q.shape
    heads = width // HD
    local = text_q.shape[0]
    devices = lax.axis_size("tile")
    groups = lax.axis_size("head")
    if groups == 2 and devices == 4 * DH and heads % 2 == 0 and rows == GT * TILE_TOK:
        return fused(
            video_q, video_k, video_v, text_q, text_k, text_v, video_proj, text_proj,
            window_mask, text_length,
        )
    chunks = max(c for c in range(1, CHUNKS + 1) if heads % c == 0)
    step = heads // chunks

    text = lax.all_gather(jnp.stack([text_q, text_k, text_v]), "tile", axis=1, tiled=True)
    nears = []
    for c in range(chunks):
        part = slice(c * step * HD, (c + 1) * step * HD)
        nears.append(halo(jnp.stack([video_k[:, part], video_v[:, part]])))

    first = (lax.axis_index("tile") * local).astype(jnp.int32).reshape(1)
    text_part, text_lse = text_attention(
        first, text_length, text[0], video_k, video_v, text_k, text_v
    )
    text_part = lax.all_to_all(
        text_part.reshape(devices, local, width), "tile", split_axis=0, concat_axis=0
    )
    text_lse = lax.all_to_all(
        text_lse.reshape(devices, local, HD), "tile", split_axis=0, concat_axis=0
    )[:, :, :heads]
    share = jax.nn.softmax(text_lse, axis=0)
    text_attn = jnp.sum(
        share[..., None] * text_part.reshape(devices, local, heads, HD).astype(jnp.float32), axis=0
    )
    text_attn = text_attn.reshape(local, width).astype(jnp.bfloat16)

    results = [
        video_attention(
            window_mask, text_length, video_q, near, text[1], text[2], c * step, step
        )
        for c, near in enumerate(nears)
    ]
    video_attn = jnp.concatenate(results, axis=1)
    return (
        project(video_attn, video_proj, groups),
        project(text_attn, text_proj, groups),
    )


def project(attn, proj, groups):
    if groups != 2:
        part = jnp.dot(attn, proj, preferred_element_type=jnp.float32).astype(jnp.bfloat16)
        return lax.psum_scatter(part, "head", scatter_dimension=1, tiled=True)
    half = proj.shape[1] // groups
    me = lax.axis_index("head")
    theirs = lax.dynamic_slice_in_dim(proj, (1 - me) * half, half, 1)
    mine = lax.dynamic_slice_in_dim(proj, me * half, half, 1)
    away = jnp.dot(attn, theirs, preferred_element_type=jnp.float32).astype(jnp.bfloat16)
    arrived = lax.ppermute(away, "head", [(0, 1), (1, 0)])
    home = jnp.dot(attn, mine, preferred_element_type=jnp.float32).astype(jnp.bfloat16)
    return (home.astype(jnp.float32) + arrived.astype(jnp.float32)).astype(jnp.bfloat16)


def fused_kernel(
    mask_ref, length_ref, q_ref, k_ref, v_ref, tq_ref, tk_ref, tv_ref, vproj_ref, tproj_ref,
    vout_ref, tout_ref,
    qb, kb, vb, tb, biasb, peakb, accb, obuf, hp, xa, wh, wa, tw, homeb, awayb, tpart, tlog, tlse,
    tpy, tly, trecv, tlrecv, ta, tsend, tarrive,
    local_sem, pair_send, pair_recv, z_send, z_recv, y_send, y_recv, fy_send, fz_send, d_recv,
    th_send, th_recv, ty_send, ty_recv, py_send, py_recv, ly_send, ly_recv,
    ta_send, ta_recv, tl_send, tl_recv,
    w_send, w_recv, wf_send, wf_recv, op_send, op_recv, ox_send, ox_recv, tx_send, tx_recv,
):
    rows, width = q_ref.shape
    half = width // 2
    heads = half // HD
    local = tq_ref.shape[0]
    text = tb.shape[1]
    out_width = vout_ref.shape[1]
    across = lax.axis_size("tile") // DH
    tiles = rows // TILE_TOK

    me = lax.axis_index("tile")
    group = lax.axis_index("head")
    r = me // across
    yc = me % across // 2
    c = me % 2
    inner = 1 - yc
    chip = r * 2 + yc
    has_lo = r > 0
    has_hi = r < DH - 1
    turned = heads // 2

    def at(row, ycol, core):
        return (row * across + 2 * ycol + core, group)

    partner = at(r, yc, 1 - c)
    mesh_id = pl.DeviceIdType.MESH

    barrier = pltpu.get_barrier_semaphore()

    def greet(device):
        pl.semaphore_signal(barrier, inc=1, device_id=device, device_id_type=mesh_id)

    def line(n):
        return at(n // 2, yc, n % 2)

    spot = 2 * r + c

    @pl.loop(0, 2 * DH)
    def _(n):
        @pl.when(n != spot)
        def _():
            greet(line(n))

    for core in range(2):
        greet(at(r, 1 - yc, core))
        greet((at(r, yc, core)[0], 1 - group))
    pl.semaphore_wait(barrier, 2 * DH + 3)
    sides = (k_ref, v_ref)
    bufs = (kb, vb)

    def lanes(h):
        return pl.ds(pl.multiple_of(h * HD, HD), HD)

    def half_lanes(core):
        return pl.ds(pl.multiple_of(core * half, HD), half)

    def remote(src, dst, send, recv, device):
        return pltpu.make_async_remote_copy(
            src_ref=src, dst_ref=dst, send_sem=send, recv_sem=recv, device_id=device,
            device_id_type=mesh_id,
        )

    def arrived(dst, recv):
        remote(dst, dst, pair_send.at[0], recv, partner).wait_recv()

    def z_copy(kv, d, core, h, f):
        slot = (2 if d else 4) + c
        part = slice(f * TILE_TOK, (f + 1) * TILE_TOK)
        return remote(
            sides[kv].at[part, lanes(core * heads + h)], bufs[kv].at[slot, part, lanes(h)],
            z_send.at[f, kv, d, core, h], z_recv.at[f, kv, slot - 2, h],
            at(r + (1 if d else -1), yc, core),
        )

    def y_copy(kv, core, h):
        return remote(
            sides[kv].at[:, lanes(core * heads + h)], bufs[kv].at[6, :, lanes(h)],
            y_send.at[kv, core, h], y_recv.at[kv, h], at(r, 1 - yc, core),
        )

    def fy_copy(kv, d, h):
        return remote(
            bufs[kv].at[(4 if d else 2) + inner, :, lanes(h)], bufs[kv].at[7 + d, :, lanes(h)],
            fy_send.at[kv, d, h], d_recv.at[kv, d, h], at(r, 1 - yc, c),
        )

    def fz_copy(kv, d, h):
        return remote(
            bufs[kv].at[6, :, lanes(h)], bufs[kv].at[7 + d, :, lanes(h)],
            fz_send.at[kv, d, h], d_recv.at[kv, d, h], at(r + (-1 if d else 1), yc, c),
        )

    def each_z(h, act):
        for f in range(GT):
            for d, ok in ((1, has_hi), (0, has_lo)):
                @pl.when(ok)
                def _():
                    for kv in range(2):
                        for core in range(2):
                            act(z_copy(kv, d, core, h, f))

    def each_y(h, act):
        @pl.when(c == inner)
        def _():
            for kv in range(2):
                for core in range(2):
                    act(y_copy(kv, core, h))

    def each_fy(h, act):
        for d, ok in ((0, has_lo), (1, has_hi)):
            @pl.when(ok & (h < turned))
            def _():
                for kv in range(2):
                    act(fy_copy(kv, d, h))

    def each_fz(h, act):
        for d, ok in ((0, has_hi), (1, has_lo)):
            @pl.when(ok & (h >= turned))
            def _():
                for kv in range(2):
                    act(fz_copy(kv, d, h))

    def start(copy):
        copy.start()

    def sent(copy):
        copy.wait_send()

    def piece(row, ycol):
        return tb.at[:, pl.ds(pl.multiple_of((row * 2 + ycol) * 2 * local, 2 * local), 2 * local), :]

    def th_copy(i, row, core):
        return remote(
            texts[i].at[:, half_lanes(core)], tb.at[i, mine, :], th_send.at[i, row, core],
            th_recv.at[i, r, c], at(row, yc, core),
        )

    def each_th(row, act):
        for core in range(2):
            for i in range(3):
                act(th_copy(i, row, core))

    def each_row(act):
        for k in range(1, DH):
            for ok, row in ((r >= k, r - k), (r + k < DH, r + k)):
                @pl.when(ok)
                def _():
                    act(row)

    def text_in(row):
        for core in range(2):
            for i in range(3):
                place = pl.ds(pl.multiple_of(at(row, yc, core)[0] * local, local), local)
                arrived(tb.at[i, place, :], th_recv.at[i, row, core])
        ty_copy(row).start()

    def ty_copy(row):
        return remote(
            piece(row, yc), piece(row, yc), ty_send.at[row], ty_recv.at[row], at(r, 1 - yc, c)
        )

    mine = pl.ds(pl.multiple_of(me * local, local), local)
    texts = (tq_ref, tk_ref, tv_ref)
    local_copies = [
        pltpu.make_async_copy(texts[i].at[:, half_lanes(c)], tb.at[i, mine, :], local_sem.at[i])
        for i in range(3)
    ]
    pair_copies = [
        remote(
            texts[i].at[:, half_lanes(1 - c)], tb.at[i, mine, :], pair_send.at[i],
            pair_recv.at[i], partner,
        )
        for i in range(3)
    ]
    for dst, src, i in ((kb.at[c], k_ref, 3), (vb.at[c], v_ref, 4), (qb.at[c], q_ref, 5)):
        local_copies.append(
            pltpu.make_async_copy(src.at[:, half_lanes(c)], dst, local_sem.at[i])
        )
        pair_copies.append(
            remote(src.at[:, half_lanes(1 - c)], dst, pair_send.at[i], pair_recv.at[i], partner)
        )
    pair_copies.append(
        remote(biasb.at[c], biasb.at[c], pair_send.at[6], pair_recv.at[6], partner)
    )
    theirs = pl.ds(pl.multiple_of((me + 1 - 2 * c) * local, local), local)
    pair_targets = [tb.at[i, theirs, :] for i in range(3)] + [
        kb.at[1 - c], vb.at[1 - c], qb.at[1 - c], biasb.at[1 - c]
    ]
    home_copy = pltpu.make_async_copy(
        vproj_ref.at[:, pl.ds(pl.multiple_of(group * out_width, HD), out_width)], wh,
        local_sem.at[6],
    )
    tw_copy = pltpu.make_async_copy(tproj_ref, tw, local_sem.at[7])
    w_rows = pl.ds(pl.multiple_of(c * half, HD), half)
    w_copy = remote(
        vproj_ref.at[w_rows, pl.ds(pl.multiple_of((1 - group) * out_width, HD), out_width)],
        wa.at[w_rows, :], w_send.at[0], w_recv.at[0], (me, 1 - group),
    )
    wf_copy = remote(wa.at[w_rows, :], wa.at[w_rows, :], wf_send.at[0], wf_recv.at[0], partner)

    for i in range(3):
        local_copies[i].start()
        pair_copies[i].start()
    each_row(lambda row: each_th(row, start))
    each_z(0, start)
    each_y(0, start)
    for i in range(3, 6):
        local_copies[i].start()
        pair_copies[i].start()
    w_copy.start()
    each_z(1, start)
    each_y(1, start)
    for t in range(tiles):
        for n in range(27):
            live = jnp.full((1, HD), mask_ref[t, n], jnp.int32) > 0
            biasb[c, 27 * t + n : 27 * t + n + 1, :] = jnp.where(live, 0.0, NEG_FILL).astype(
                jnp.float32
            )
    for i in range(3):
        local_copies[i].wait()
        arrived(pair_targets[i], pair_recv.at[i])
    ty_copy(r).start()
    pair_copies[6].start()
    for i in range(3, 6):
        local_copies[i].wait()
    for i in range(3, 7):
        arrived(pair_targets[i], pair_recv.at[i])
    home_copy.start()
    tw_copy.start()
    length = length_ref[0]

    def turn(values):
        return jnp.concatenate(
            [values.T, jnp.ones((16, values.shape[0]), values.dtype)], axis=0
        )

    def attend(h, q, blocks, with_text, first_group, frames=tuple(range(GT))):
        hs = lanes(h)
        keys_of = slice(frames[0] * TILE_TOK, (frames[-1] + 1) * TILE_TOK)
        values = [turn(vb[slot, keys_of, hs]) for slot, _, _ in blocks]
        if with_text:
            text_values = turn(tb[2, :, hs])
        for t in range(tiles):
            queries = qb[q, t * TILE_TOK : (t + 1) * TILE_TOK, hs]
            parts = []
            maxima = []
            for (slot, row_gap, col_gap), value in zip(blocks, values):
                scores = dot_nt(kb[slot, keys_of, hs], queries)
                for n, f in enumerate(frames):
                    column = 27 * t + 9 * (f - t + 1) + 3 * (row_gap + 1) + col_gap + 1
                    bias = biasb[q, pl.ds(column, 1), :]
                    bias = jnp.concatenate([bias] * (TILE_TOK // HD), axis=1)
                    part = scores[n * TILE_TOK : (n + 1) * TILE_TOK]
                    maxima.append(jnp.max(part, axis=0, keepdims=True) + bias)
                    parts.append((part, bias, value))
            if with_text:
                scores = dot_nt(tb[1, :, hs], queries)
                live = lax.broadcasted_iota(jnp.int32, scores.shape, 0) < length
                scores = jnp.where(live, scores, NEG_FILL)
                maxima.append(jnp.max(scores, axis=0, keepdims=True))
            peak = functools.reduce(jnp.maximum, maxima)
            if not first_group:
                old = peakb[h, q, t, 0:1, :]
                peak = jnp.maximum(old, peak)
            shift = peak * SCALE2
            total = None
            for n in range(0, len(parts), len(frames)):
                weights = [
                    jnp.exp2(p * SCALE2 - (shift - b)).astype(jnp.bfloat16)
                    for p, b, _ in parts[n : n + len(frames)]
                ]
                term = jnp.dot(
                    parts[n][2], jnp.concatenate(weights, axis=0),
                    preferred_element_type=jnp.float32,
                )
                total = term if total is None else total + term
            if with_text:
                weights = jnp.exp2(scores * SCALE2 - shift).astype(jnp.bfloat16)
                total = total + jnp.dot(
                    text_values, weights, preferred_element_type=jnp.float32
                )
            if not first_group:
                total = accb[h, q, t] * jnp.exp2(old * SCALE2 - shift) + total
            accb[h, q, t] = total
            peakb[h, q, t, 0:1, :] = peak

    @pl.loop(0, heads)
    def _(h):
        @pl.when(h == heads // 2)
        def _():
            each_row(text_in)
            for g in range(2, turned):
                each_z(g, start)
                each_y(g, start)

        @pl.loop(0, 2)
        def _(q):
            attend(h, q, [(0, 0, -q), (1, 0, 1 - q)], False, True)

    for row in range(DH):
        arrived(piece(row, 1 - yc), ty_recv.at[row])

    first = chip * 2 * local
    tlog[...] = jnp.zeros_like(tlog)

    @pl.loop(0, heads)
    def _(h):
        queries = tb[0, :, lanes(h)]
        scores = [dot_nt(keys, queries) for keys in (kb[0, :, lanes(h)], kb[1, :, lanes(h)])]
        own = dot_nt(tb[1, :, lanes(h)], queries)
        index = lax.broadcasted_iota(jnp.int32, own.shape, 0)
        live = (index >= first) & (index < first + 2 * local) & (index < length)
        scores.append(jnp.where(live, own, NEG_FILL))
        peak = functools.reduce(
            jnp.maximum, [jnp.max(s, axis=0, keepdims=True) for s in scores]
        )
        weights = [jnp.exp2((s - peak) * SCALE2) for s in scores]
        total = sum(jnp.sum(w, axis=0, keepdims=True) for w in weights)
        values = [vb[0, :, lanes(h)], vb[1, :, lanes(h)], tb[2, :, lanes(h)]]
        acc = sum(
            jnp.dot(v.T, w.astype(jnp.bfloat16), preferred_element_type=jnp.float32)
            for w, v in zip(weights, values)
        )
        tpart[:, lanes(h)] = (acc / total).T.astype(jnp.bfloat16)
        tlog[pl.ds(h, 1), :] = peak * SCALE + jnp.log(total)

    tlse[...] = tlog[...].T

    def piece_rows(row, ycol):
        return pl.ds(pl.multiple_of((row * 2 + ycol) * 2 * local, 2 * local), 2 * local)

    def over_copies(row):
        away = piece_rows(row, 1 - yc)
        device = at(r, 1 - yc, c)
        return (
            remote(tpart.at[away, :], tpy.at[row], py_send.at[row], py_recv.at[row], device),
            remote(tlse.at[away, :], tly.at[row], ly_send.at[row], ly_recv.at[row], device),
        )

    for row in range(DH):
        for copy in over_copies(row):
            copy.start()

    def part_copies(n):
        rows_ = pl.ds(pl.multiple_of(line(n)[0] * local, local), local)
        return (
            remote(tpart.at[rows_, :], trecv.at[r, c], ta_send.at[n], ta_recv.at[r, c], line(n)),
            remote(tlse.at[rows_, :], tlrecv.at[r, c], tl_send.at[n], tl_recv.at[r, c], line(n)),
        )

    def join_text():
        for row in range(DH):
            arrived(tpy.at[row], py_recv.at[row])
            arrived(tly.at[row], ly_recv.at[row])
            here = piece_rows(row, yc)
            first_, second = tlse[here, :], tly[row]
            top = jnp.maximum(first_, second)
            first_, second = jnp.exp(first_ - top), jnp.exp(second - top)
            whole = first_ + second
            tlse[here, :] = top + jnp.log(whole)
            first_, second = first_ / whole, second / whole
            for j in range(heads):
                cols = slice(j * HD, (j + 1) * HD)
                tpart[here, cols] = (
                    first_[:, j : j + 1] * tpart[here, cols].astype(jnp.float32)
                    + second[:, j : j + 1] * tpy[row, :, cols].astype(jnp.float32)
                ).astype(jnp.bfloat16)
        trecv[r, c] = tpart[mine, :]
        tlrecv[r, c] = tlse[mine, :]

        @pl.loop(0, 2 * DH)
        def _(n):
            @pl.when(n != spot)
            def _():
                for copy in part_copies(n):
                    copy.start()

    def op_copy(h):
        return remote(
            obuf.at[1 - c, :, lanes(h)], hp.at[:, lanes(h)], op_send.at[h], op_recv.at[h], partner
        )

    def ox_copy(core, h):
        return remote(
            obuf.at[core, :, lanes(h)], xa.at[c, :, lanes(h)], ox_send.at[core, h],
            ox_recv.at[c, h], (at(r, yc, core)[0], 1 - group),
        )

    tx_copy = remote(
        tsend, tarrive, tx_send.at[0], tx_recv.at[0], (me, 1 - group)
    )

    def finish_text():
        @pl.loop(0, 2 * DH)
        def _(n):
            @pl.when(n != spot)
            def _():
                arrived(trecv.at[n // 2, n % 2], ta_recv.at[n // 2, n % 2])
                arrived(tlrecv.at[n // 2, n % 2], tl_recv.at[n // 2, n % 2])

        for core in range(2):
            lse = [tlrecv[s, core] for s in range(DH)]
            top = functools.reduce(jnp.maximum, lse)
            share = [jnp.exp(l - top) for l in lse]
            whole = sum(share)
            share = [s / whole for s in share]
            for j in range(heads):
                cols = slice(j * HD, (j + 1) * HD)
                acc = sum(
                    share[s][:, j : j + 1] * trecv[s, core, :, cols].astype(jnp.float32)
                    for s in range(DH)
                )
                ta[:, core * half + j * HD : core * half + (j + 1) * HD] = acc.astype(jnp.bfloat16)
        tw_copy.wait()

        @pl.loop(0, out_width // half)
        def _(n):
            cols = pl.ds(pl.multiple_of(n * half, HD), half)
            away = pl.ds(pl.multiple_of((1 - group) * out_width + n * half, HD), half)
            tsend[:, cols] = jnp.dot(
                ta[...], tw[:, away], preferred_element_type=jnp.float32
            ).astype(jnp.bfloat16)

        tx_copy.start()

    def out_part(h, q):
        for t in range(tiles):
            acc = accb[h, q, t]
            obuf[q, t * TILE_TOK : (t + 1) * TILE_TOK, lanes(h)] = (
                (acc[:HD] / acc[HD : HD + 1]).T.astype(jnp.bfloat16)
            )
        ox_copy(q, h).start()

        @pl.when(q != c)
        def _():
            op_copy(h).start()

    def y_in(h):
        for kv in range(2):
            arrived(bufs[kv].at[6, :, lanes(h)], y_recv.at[kv, h])

    def z_in(h, f):
        part = slice(f * TILE_TOK, (f + 1) * TILE_TOK)
        for ok, slots in ((has_lo, (2, 3)), (has_hi, (4, 5))):
            @pl.when(ok)
            def _():
                for kv in range(2):
                    for slot in slots:
                        arrived(
                            bufs[kv].at[slot, part, lanes(h)], z_recv.at[f, kv, slot - 2, h]
                        )

    def heads_in(h):
        arrived(hp.at[:, lanes(h)], op_recv.at[h])
        for core in range(2):
            arrived(xa.at[core, :, lanes(h)], ox_recv.at[core, h])

    edges = (
        (has_lo & has_hi, ((2, -1), (4, 1)), (7, 8)),
        (has_lo & jnp.logical_not(has_hi), ((2, -1),), (7,)),
        (has_hi & jnp.logical_not(has_lo), ((4, 1),), (8,)),
    )
    side = 1 - 2 * yc

    def attend_rows(h, q):
        for ok, ends, _ in edges:
            @pl.when(ok)
            def _():
                blocks = []
                for slot, gap in ends:
                    blocks += [(slot, gap, -q), (slot + 1, gap, 1 - q)]
                attend(h, q, blocks, True, False)

    def attend_side(h):
        for ok, _, corners in edges:
            @pl.when(ok)
            def _():
                for slot in corners:
                    for kv in range(2):
                        arrived(bufs[kv].at[slot, :, lanes(h)], d_recv.at[kv, slot - 7, h])
                blocks = [(6, 0, side)] + [(slot, 2 * slot - 15, side) for slot in corners]
                attend(h, inner, blocks, False, False)

    early = turned * HD

    def project(cols, from_, to):
        span = slice(from_, to)
        size = to - from_
        mine_ = pl.ds(pl.multiple_of(c * half + from_, HD), size)
        other = pl.ds(pl.multiple_of((1 - c) * half + from_, HD), size)
        home = jnp.dot(obuf[c, :, span], wh[mine_, cols], preferred_element_type=jnp.float32)
        home = home + jnp.dot(hp[:, span], wh[other, cols], preferred_element_type=jnp.float32)
        away = jnp.dot(xa[0, :, span], wa[span, cols], preferred_element_type=jnp.float32)
        away = away + jnp.dot(
            xa[1, :, span], wa[half + from_ : half + to, cols],
            preferred_element_type=jnp.float32,
        )
        return home, away

    def project_early():
        home_copy.wait()
        arrived(wa.at[other_rows, :], wf_recv.at[0])

        @pl.loop(0, turned)
        def _(h):
            heads_in(h)

        @pl.loop(0, out_width // TILE_TOK)
        def _(n):
            cols = pl.ds(pl.multiple_of(n * TILE_TOK, HD), TILE_TOK)
            homeb[:, cols], awayb[:, cols] = project(cols, 0, early)

    def text_out():
        arrived(tarrive, tx_recv.at[0])

        @pl.loop(0, out_width // half)
        def _(n):
            cols = pl.ds(pl.multiple_of(n * half, HD), half)
            here = pl.ds(pl.multiple_of(group * out_width + n * half, HD), half)
            home = jnp.dot(ta[...], tw[:, here], preferred_element_type=jnp.float32)
            tout_ref[:, cols] = (
                home.astype(jnp.bfloat16).astype(jnp.float32)
                + tarrive[:, cols].astype(jnp.float32)
            ).astype(jnp.bfloat16)

    other_rows = pl.ds(pl.multiple_of((1 - c) * half, HD), half)

    @pl.loop(0, heads)
    def _(h):
        @pl.when(h + turned < heads)
        def _():
            each_y(h + turned, start)

        @pl.when((h + 2 >= turned) & (h + 2 < heads))
        def _():
            y_in(h + 2)
            each_fz(h + 2, start)
            each_z(h + 2, start)

        @pl.when(h < turned)
        def _():
            for f in range(GT):
                z_in(h, f)
            each_fy(h, start)

            @pl.loop(0, 2)
            def _(q):
                attend_rows(h, q)

        @pl.when(h == 1)
        def _():
            join_text()

        low = jnp.where(h <= turned, jnp.maximum(h - 1, 0), h)
        high = jnp.where(h < turned, h, h + 1)

        @pl.loop(low, high)
        def _(g):
            @pl.when(g < turned)
            def _():
                y_in(g)

            attend_side(g)

            @pl.when(g < turned)
            def _():
                @pl.loop(0, 2)
                def _(q):
                    out_part(g, q)

        @pl.when(h == heads // 2)
        def _():
            arrived(wa.at[w_rows, :], w_recv.at[0])
            wf_copy.start()

        @pl.when(h == heads - 2)
        def _():
            finish_text()

        @pl.when(h == heads - 1)
        def _():
            text_out()
            project_early()

        @pl.when(h >= turned)
        def _():
            for f in range(GT):
                z_in(h, f)

            @pl.loop(0, 2)
            def _(q):
                attend_rows(h, q)
                out_part(h, q)

    for h in range(turned, heads):
        heads_in(h)

    @pl.loop(0, out_width // TILE_TOK)
    def _(n):
        cols = pl.ds(pl.multiple_of(n * TILE_TOK, HD), TILE_TOK)
        home, away = project(cols, early, half)
        home = home + homeb[:, cols]
        away = away + awayb[:, cols]
        vout_ref[:, cols] = (
            home.astype(jnp.bfloat16).astype(jnp.float32)
            + away.astype(jnp.bfloat16).astype(jnp.float32)
        ).astype(jnp.bfloat16)

    for copy in pair_copies:
        copy.wait_send()
    w_copy.wait_send()
    wf_copy.wait_send()
    tx_copy.wait_send()
    for row in range(DH):
        ty_copy(row).wait_send()
    each_row(lambda row: each_th(row, sent))

    for row in range(DH):
        for copy in over_copies(row):
            copy.wait_send()

    @pl.loop(0, 2 * DH)
    def _(n):
        @pl.when(n != spot)
        def _():
            for copy in part_copies(n):
                copy.wait_send()

    @pl.loop(0, heads)
    def _(h):
        each_z(h, sent)
        each_y(h, sent)
        each_fy(h, sent)
        each_fz(h, sent)
        ox_copy(0, h).wait_send()
        ox_copy(1, h).wait_send()
        op_copy(h).wait_send()


def fused(
    video_q, video_k, video_v, text_q, text_k, text_v, video_proj, text_proj, window_mask,
    text_length,
):
    rows, width = video_q.shape
    half = width // 2
    heads = half // HD
    local = text_q.shape[0]
    devices = lax.axis_size("tile")
    text = devices * local
    out_width = video_proj.shape[1] // lax.axis_size("head")
    tiles = rows // TILE_TOK
    slots = -(-window_mask.size // 8) * 8
    bf16 = jnp.bfloat16
    f32 = jnp.float32
    anywhere = pl.BlockSpec(memory_space=pl.ANY)
    vmem = pl.BlockSpec(memory_space=pltpu.VMEM)
    dma = pltpu.SemaphoreType.DMA
    return pl.pallas_call(
        fused_kernel,
        in_specs=[pl.BlockSpec(memory_space=pltpu.SMEM)] * 2 + [anywhere] * 8,
        out_specs=[vmem, vmem],
        out_shape=[
            jax.ShapeDtypeStruct((rows, out_width), bf16),
            jax.ShapeDtypeStruct((local, out_width), bf16),
        ],
        scratch_shapes=[
            pltpu.VMEM((2, rows, half), bf16),
            pltpu.VMEM((9, rows, half), bf16),
            pltpu.VMEM((9, rows, half), bf16),
            pltpu.VMEM((3, text, half), bf16),
            pltpu.VMEM((2, slots, HD), f32),
            pltpu.VMEM((heads, 2, tiles, 8, TILE_TOK), f32),
            pltpu.VMEM((heads, 2, tiles, HD + 16, TILE_TOK), f32),
            pltpu.VMEM((2, rows, half), bf16),
            pltpu.VMEM((rows, half), bf16),
            pltpu.VMEM((2, rows, half), bf16),
            pltpu.VMEM((width, out_width), bf16),
            pltpu.VMEM((width, out_width), bf16),
            pltpu.VMEM(text_proj.shape, bf16),
            pltpu.VMEM((rows, out_width), f32),
            pltpu.VMEM((rows, out_width), f32),
            pltpu.VMEM((text, half), bf16),
            pltpu.VMEM((HD, text), f32),
            pltpu.VMEM((text, HD), f32),
            pltpu.VMEM((DH, 2 * local, half), bf16),
            pltpu.VMEM((DH, 2 * local, HD), f32),
            pltpu.VMEM((DH, 2, local, half), bf16),
            pltpu.VMEM((DH, 2, local, HD), f32),
            pltpu.VMEM((local, width), bf16),
            pltpu.VMEM((local, out_width), bf16),
            pltpu.VMEM((local, out_width), bf16),
            dma((8,)), dma((7,)), dma((7,)),
            dma((GT, 2, 2, 2, heads)), dma((GT, 2, 4, heads)),
            dma((2, 2, heads)), dma((2, heads)),
            dma((2, 2, heads)), dma((2, 2, heads)), dma((2, 2, heads)),
            dma((3, DH, 2)), dma((3, DH, 2)), dma((DH,)), dma((DH,)),
            dma((DH,)), dma((DH,)), dma((DH,)), dma((DH,)),
            dma((2 * DH,)), dma((DH, 2)), dma((2 * DH,)), dma((DH, 2)),
            dma((1,)), dma((1,)), dma((1,)), dma((1,)),
            dma((heads,)), dma((heads,)), dma((2, heads)), dma((2, heads)),
            dma((1,)), dma((1,)),
        ],
        compiler_params=pltpu.CompilerParams(
            vmem_limit_bytes=63 * 1024 * 1024, has_side_effects=True, collective_id=0
        ),
        name="fused",
    )(
        window_mask, text_length, video_q, video_k, video_v, text_q, text_k, text_v, video_proj,
        text_proj,
    )


def solution(mesh):
    placed = (P("tile", "head"),) * 6 + (P("head", None),) * 2 + (P("tile", None), P())
    return jax.shard_map(
        per_device,
        mesh=mesh,
        in_specs=placed,
        out_specs=(P("tile", "head"), P("tile", "head")),
        check_vma=False,
    )
```
